16 devices in a mesh: dp: 2 (over y, z), ep: 8 (over x, core).
Axes of the slice: x: 4, y: 2, z: 1, core: 2. Of those that a mesh axis runs over, the one named last changes fastest.
The devices are a block of a 4x4x8 slice.
Arguments:
- tokens: bfloat16 [2048, 2048], P(('dp', 'ep')), parts along dimension 0
- routes: int32 [2048, 8], P(('dp', 'ep')), parts along dimension 0
- w_router: bfloat16 [2048, 64], replicated
- w_one: bfloat16 [64, 2048, 1024], P('ep')
- w_three: bfloat16 [64, 2048, 1024], P('ep')
- w_two: bfloat16 [64, 1024, 2048], P('ep')
Outputs:
- output: bfloat16 [2048, 2048], P(('dp', 'ep')), parts along dimension 0
There are 2 independent parts. The reference program is written for one: setup_inputs(seed, part) draws one part's arguments, and reference() takes and returns one part's arrays. A program takes and returns all parts, laid end to end along the dimension named above; an argument that names none is the same for every part.
All inputs are finite; a program needn't handle non-finite values.
Results may differ from the reference program's by a relative error of at most 0.00817308.
Values are sent between devices in bfloat16 or wider.
A program may use at most 768 MiB of HBM per device.

```python
import jax
import jax.numpy as jnp
from jax import lax

GROUP_SIZE = 8
DEV_TOKENS = 128
D_MODEL = 2048
D_EXPERT = 1024
NUM_EXPERTS = 64
TOP_K = 8
CAPACITY = 24


def draw_routes(route_key):
    perm_key, row_key, slot_key = jax.random.split(route_key, 3)
    num_pairs = DEV_TOKENS * TOP_K
    hot_count = NUM_EXPERTS // 8
    rest_pairs = num_pairs - hot_count * CAPACITY
    base_count = rest_pairs // (NUM_EXPERTS - hot_count)
    extra_count = rest_pairs % (NUM_EXPERTS - hot_count)
    rank_ids = jnp.arange(NUM_EXPERTS, dtype=jnp.int32)
    counts = jnp.where(rank_ids < hot_count, CAPACITY, base_count + (rank_ids - hot_count < extra_count).astype(jnp.int32))
    count_ends = jnp.cumsum(counts)
    pair_rank = jnp.searchsorted(count_ends, jnp.arange(num_pairs, dtype=jnp.int32), side='right')
    expert_of_rank = jax.random.permutation(perm_key, NUM_EXPERTS)
    layout = expert_of_rank[pair_rank].reshape(TOP_K, DEV_TOKENS).T

    def device_routes(perm_rows, perm_slots):
        row_order = jax.random.permutation(perm_rows, DEV_TOKENS)
        scores = jax.random.randint(perm_slots, (DEV_TOKENS, TOP_K), 0, 1 << 20) * TOP_K + jnp.arange(TOP_K)
        slot_order = jnp.argsort(scores, axis=1)
        return jnp.take_along_axis(layout[row_order], slot_order, axis=1)

    per_device = jax.vmap(device_routes)(jax.random.split(row_key, GROUP_SIZE), jax.random.split(slot_key, GROUP_SIZE))
    return per_device.reshape(GROUP_SIZE * DEV_TOKENS, TOP_K).astype(jnp.int32)


def setup_inputs(seed: int = 0, part: int = 0) -> dict:
    part_key = jax.random.fold_in(jax.random.key(seed), part)
    token_key, route_key = jax.random.split(part_key)
    shared = jax.random.split(jax.random.key(seed + 1), 4)
    tokens = jax.random.normal(token_key, (GROUP_SIZE * DEV_TOKENS, D_MODEL), jnp.float32)
    w_router = jax.random.normal(shared[0], (D_MODEL, NUM_EXPERTS), jnp.float32) * (1.5 * D_MODEL ** -0.5)
    w_one = jax.random.normal(shared[1], (NUM_EXPERTS, D_MODEL, D_EXPERT), jnp.float32) * D_MODEL ** -0.5
    w_three = jax.random.normal(shared[2], (NUM_EXPERTS, D_MODEL, D_EXPERT), jnp.float32) * D_MODEL ** -0.5
    w_two = jax.random.normal(shared[3], (NUM_EXPERTS, D_EXPERT, D_MODEL), jnp.float32) * D_EXPERT ** -0.5
    return {'tokens': tokens.astype(jnp.bfloat16), 'routes': draw_routes(route_key), 'w_router': w_router.astype(jnp.bfloat16), 'w_one': w_one.astype(jnp.bfloat16), 'w_three': w_three.astype(jnp.bfloat16), 'w_two': w_two.astype(jnp.bfloat16)}


def expert_rows(rows, w_gate, w_up, w_down):
    gate_pre = jnp.dot(rows, w_gate, preferred_element_type=jnp.float32)
    up_pre = jnp.dot(rows, w_up, preferred_element_type=jnp.float32)
    hidden = (jax.nn.silu(gate_pre) * up_pre).astype(jnp.bfloat16)
    return jnp.dot(hidden, w_down, preferred_element_type=jnp.float32).astype(jnp.bfloat16)


def reference(tokens, routes, w_router, w_one, w_three, w_two):
    logits = jnp.dot(tokens, w_router, preferred_element_type=jnp.float32)
    gate_vals = jax.nn.softmax(jnp.take_along_axis(logits, routes, axis=1), axis=-1)
    flat_gates = gate_vals.reshape(-1)
    flat_routes = routes.reshape(-1)
    num_pairs = flat_routes.shape[0]
    sort_order = jnp.argsort(flat_routes, stable=True)
    counts = jax.ops.segment_sum(jnp.ones_like(flat_routes), flat_routes, num_segments=NUM_EXPERTS)
    starts = jnp.cumsum(counts) - counts
    slot_ids = jnp.arange(GROUP_SIZE * CAPACITY, dtype=jnp.int32)

    def one_expert(y_sum, step_in):
        w_gate, w_up, w_down, exp_start, exp_count = step_in
        pair_at = sort_order[jnp.minimum(exp_start + slot_ids, num_pairs - 1)]
        token_at = pair_at // TOP_K
        weight = jnp.where(slot_ids < exp_count, flat_gates[pair_at], 0.0)
        out_rows = expert_rows(tokens[token_at], w_gate, w_up, w_down)
        return y_sum.at[token_at].add(weight[:, None] * out_rows.astype(jnp.float32)), None

    y_sum = lax.scan(one_expert, jnp.zeros(tokens.shape, jnp.float32), (w_one, w_three, w_two, starts, counts))[0]
    return y_sum.astype(jnp.bfloat16)
```

```python
import functools

import jax
import jax.numpy as jnp
from jax import lax
from jax.experimental import pallas as pl
from jax.experimental.pallas import tpu as pltpu
from jax.sharding import PartitionSpec as P

MESH = pl.DeviceIdType.MESH
F32 = jnp.float32
BF16 = jnp.bfloat16

IN_CHUNKS = 4
OUT_CHUNKS = 8
W_SLOTS = 8
OWN_SLOTS = 4
UNROLL_IN = 2
UNROLL_OUT = 2


def slot_capacity(num_tokens, top_k, num_experts):
    return 8 * ((3 * num_tokens * top_k + 16 * num_experts - 1) // (16 * num_experts))


def moe_kernel(
    cap, tokens, routes, w_router, w_one, w_three, w_two, out,
    xs, us, acc_a, acc_b, hid, w1_buf, w3_buf, w2_buf, o_buf, pick, gate_mat,
    s_loc, g_loc, s_all, g_all, own, p_send, p_recv, h_recv, f_recv,
    tok_sem, w1_sem, w3_sem, w2_sem, ag_send, ag_recv, s_send, s_recv, g_send, g_recv,
    ps_sem, pr_sem, hs_sem, hr_sem, fs_sem, fr_sem,
):
    num_tokens, d_model = tokens.shape
    top_k = routes.shape[1]
    num_experts = w_router.shape[1]
    local_experts = w_one.shape[0]
    num_dev = num_experts // local_experts
    num_chips = num_dev // 2
    kc = d_model // IN_CHUNKS
    nw = d_model // OUT_CHUNKS
    rows = num_dev * cap
    slots = local_experts * cap
    half = num_tokens // 2

    me = lax.axis_index("ep")
    chip = me // 2
    core = lax.rem(me, 2)

    def at_chip(k):
        return lax.rem(chip + k, num_chips)

    right = at_chip(1) * 2 + core
    left = at_chip(num_chips - 1) * 2 + core
    opp = at_chip(2) * 2 + core
    partner = chip * 2 + 1 - core

    def w_copies(step):
        i = step // local_experts
        e = lax.rem(step, local_experts)
        slot = lax.rem(step, W_SLOTS)
        rng = pl.ds(pl.multiple_of(i * kc, kc), kc)
        return (
            pltpu.make_async_copy(w_one.at[e, rng, :], w1_buf.at[slot], w1_sem.at[slot]),
            pltpu.make_async_copy(w_three.at[e, rng, :], w3_buf.at[slot], w3_sem.at[slot]),
        )

    def w_start(step):
        for copy in w_copies(step):
            copy.start()

    def w2_copy(n):
        return pltpu.make_async_copy(
            w_two.at[:, :, pl.ds(n * nw, nw)], w2_buf.at[n % 2], w2_sem.at[n % 2]
        )

    def tok_copy(i):
        return pltpu.make_async_copy(
            tokens.at[:, pl.ds(i * kc, kc)], xs.at[i, me], tok_sem.at[i]
        )

    for i in range(IN_CHUNKS):
        tok_copy(i).start()
    for step in range(W_SLOTS):
        w_start(jnp.int32(step))

    barrier = pltpu.get_barrier_semaphore()
    for k in range(1, num_dev):
        pl.semaphore_signal(
            barrier, inc=1, device_id={"ep": lax.rem(me + k, num_dev)}, device_id_type=MESH
        )

    expert_id = lax.broadcasted_iota(jnp.int32, (num_tokens, num_experts), 1)
    member = jnp.zeros((num_tokens, num_experts), F32)
    for j in range(top_k):
        member = member + jnp.where(routes[:, j : j + 1] == expert_id, 1.0, 0.0)
    row_id = lax.broadcasted_iota(jnp.int32, (num_tokens, num_tokens), 0)
    col_id = lax.broadcasted_iota(jnp.int32, (num_tokens, num_tokens), 1)
    before = jnp.where(col_id < row_id, 1.0, 0.0).astype(BF16)
    rank = jnp.dot(before, member.astype(BF16), preferred_element_type=F32)
    slot_of = jnp.where(member > 0.5, rank, -1.0)
    s_loc[...] = slot_of.T.reshape(num_dev, local_experts, num_tokens)
    s_all[me] = s_loc[me]

    pl.semaphore_wait(barrier, num_dev - 1)

    def plan_copy(k, src, dst, send, recv):
        peer = lax.rem(me + k, num_dev)
        return pltpu.make_async_remote_copy(
            src_ref=src.at[peer], dst_ref=dst.at[me], send_sem=send.at[k - 1],
            recv_sem=recv.at[k - 1], device_id={"ep": peer}, device_id_type=MESH,
        )

    for k in range(1, num_dev):
        plan_copy(k, s_loc, s_all, s_send, s_recv).start()

    low, high, full = pl.ds(0, half), pl.ds(half, half), pl.ds(0, num_tokens)
    ag_table = (
        (me, full, right), (me, full, left), (me, full, partner),
        (left, low, right), (right, high, left),
        (left, full, partner), (right, full, partner),
        (opp, low, partner), (opp, high, partner),
    )

    def ag(i, kind):
        block, rng, dest = ag_table[kind]
        ref = xs.at[i, block, rng, :]
        return pltpu.make_async_remote_copy(
            src_ref=ref, dst_ref=ref, send_sem=ag_send.at[i, kind],
            recv_sem=ag_recv.at[i, kind], device_id={"ep": dest}, device_id_type=MESH,
        )

    def ag_own(i):
        if i < IN_CHUNKS:
            for kind in (0, 1, 2):
                ag(i, kind).start()

    def ag_stage1(i):
        if i < IN_CHUNKS:
            ag(i, 0).wait_recv()
            ag(i, 3).start()
            ag(i, 5).start()
            ag(i, 1).wait_recv()
            ag(i, 4).start()
            ag(i, 6).start()
            ag_own(i + 2)

    def ag_stage2(i):
        if i < IN_CHUNKS:
            ag(i, 3).wait_recv()
            ag(i, 7).start()
            ag(i, 4).wait_recv()
            ag(i, 8).start()

    def ag_stage3(i):
        if i < IN_CHUNKS:
            for kind in (2, 5, 6, 7, 8):
                ag(i, kind).wait_recv()

    for i in range(IN_CHUNKS):
        tok_copy(i).wait()
    ag_own(0)
    ag_own(1)

    logits = jnp.dot(xs[0, me], w_router[0:kc, :], preferred_element_type=F32)
    for i in range(1, IN_CHUNKS):
        logits = logits + jnp.dot(
            xs[i, me], w_router[i * kc : (i + 1) * kc, :], preferred_element_type=F32
        )
    chosen = member > 0.5
    peak = jnp.max(jnp.where(chosen, logits, -jnp.inf), axis=1, keepdims=True)
    powers = jnp.where(chosen, jnp.exp(jnp.where(chosen, logits - peak, 0.0)), 0.0)
    gates = powers / jnp.sum(powers, axis=1, keepdims=True)
    g_loc[...] = gates.T.reshape(num_dev, local_experts, num_tokens)
    g_all[me] = g_loc[me]
    for k in range(1, num_dev):
        plan_copy(k, g_loc, g_all, g_send, g_recv).start()

    slot_id = lax.broadcasted_iota(jnp.int32, (cap, num_tokens), 0).astype(F32)
    for k in range(1, num_dev):
        plan_copy(k, s_loc, s_all, s_send, s_recv).wait_recv()

    def build_pick(q, carry):
        parts = [
            jnp.where(s_all[q, e : e + 1, :] == slot_id, 1.0, 0.0) for e in range(local_experts)
        ]
        pick[q] = jnp.concatenate(parts, axis=0).astype(BF16)
        return carry

    lax.fori_loop(0, num_dev, build_pick, 0)

    def build_gates(q, carry):
        parts = [
            jnp.where(s_all[q, e : e + 1, :] == slot_id, g_all[q, e : e + 1, :], 0.0)
            for e in range(local_experts)
        ]
        mat = jnp.concatenate(parts, axis=0).T
        top = mat.astype(BF16)
        rest = mat - top.astype(F32)
        mid = rest.astype(BF16)
        gate_mat[q, 0] = top
        gate_mat[q, 1] = mid
        gate_mat[q, 2] = (rest - mid.astype(F32)).astype(BF16)
        return carry

    def gather(i):
        def one_source(q, carry):
            picked = jnp.dot(pick[q], xs[i, q], preferred_element_type=F32)
            base = pl.multiple_of(q * cap, 8)
            us[:, pl.ds(base, cap), :] = picked.reshape(local_experts, cap, kc)
            return carry

        lax.fori_loop(0, num_dev, one_source, 0, unroll=2)

    def experts(i, lo, hi):
        def one_expert(e):
            step = i * local_experts + e
            slot = lax.rem(step, W_SLOTS)
            c1, c3 = w_copies(step)
            u = us[e].astype(BF16)
            c1.wait()
            a = jnp.dot(u, w1_buf[slot], preferred_element_type=F32)
            if i > 0:
                a = a + acc_a[e]
            c3.wait()
            b = jnp.dot(u, w3_buf[slot], preferred_element_type=F32)
            if i > 0:
                b = b + acc_b[e]
            if i < IN_CHUNKS - 1:
                acc_a[e] = a
                acc_b[e] = b
            else:
                hid[e] = (jax.nn.silu(a) * b).astype(BF16)
            if (i + 1) * local_experts <= IN_CHUNKS * local_experts - W_SLOTS:
                w_start(step + W_SLOTS)

        def body(t, carry):
            for r in range(UNROLL_IN):
                one_expert(lo + t * UNROLL_IN + r)
            return carry

        lax.fori_loop(0, (hi - lo) // UNROLL_IN, body, 0)

    ag_stage1(0)
    ag_stage2(0)
    ag_stage3(0)
    mid_expert = local_experts // 2
    for i in range(IN_CHUNKS):
        gather(i)
        if i == IN_CHUNKS - 1:
            w2_copy(0).start()
            w2_copy(1).start()
        experts(i, 0, mid_expert)
        ag_stage1(i + 1)
        if i == 1:
            for k in range(1, num_dev):
                plan_copy(k, g_loc, g_all, g_send, g_recv).wait_recv()
            lax.fori_loop(0, num_dev, build_gates, 0)
        experts(i, mid_expert, local_experts)
        ag_stage2(i + 1)
        ag_stage3(i + 1)

    def partial(q):
        base = pl.multiple_of(q * cap, 8)
        o_rows = o_buf[:, pl.ds(base, cap), :].reshape(slots, nw).astype(BF16)
        total = jnp.dot(gate_mat[q, 2], o_rows, preferred_element_type=F32)
        total = total + jnp.dot(gate_mat[q, 1], o_rows, preferred_element_type=F32)
        return total + jnp.dot(gate_mat[q, 0], o_rows, preferred_element_type=F32)

    def p_copy(n):
        return pltpu.make_async_remote_copy(
            src_ref=p_send.at[n % 2], dst_ref=p_recv.at[n], send_sem=ps_sem.at[n],
            recv_sem=pr_sem.at[n], device_id={"ep": partner}, device_id_type=MESH,
        )

    def h_copy(n, d):
        return pltpu.make_async_remote_copy(
            src_ref=own.at[n % OWN_SLOTS, 2, low if d == 0 else high, :],
            dst_ref=h_recv.at[n, d], send_sem=hs_sem.at[n, d], recv_sem=hr_sem.at[n, d],
            device_id={"ep": right if d == 0 else left}, device_id_type=MESH,
        )

    def f_copy(n, d):
        return pltpu.make_async_remote_copy(
            src_ref=own.at[n % OWN_SLOTS, 1 if d == 0 else 3],
            dst_ref=f_recv.at[n, d], send_sem=fs_sem.at[n, d], recv_sem=fr_sem.at[n, d],
            device_id={"ep": right if d == 0 else left}, device_id_type=MESH,
        )

    def produce(n):
        if n >= 2:
            p_copy(n - 2).wait_send()
        if n >= OWN_SLOTS:
            for d in (0, 1):
                h_copy(n - OWN_SLOTS, d).wait_send()
                f_copy(n - OWN_SLOTS, d).wait_send()
        w2_copy(n).wait()

        def body(t, carry):
            for r in range(UNROLL_OUT):
                e = t * UNROLL_OUT + r
                o_buf[e] = jnp.dot(hid[e], w2_buf[n % 2, e], preferred_element_type=F32)
            return carry

        lax.fori_loop(0, local_experts // UNROLL_OUT, body, 0)
        if n + 2 < OUT_CHUNKS:
            w2_copy(n + 2).start()

        def for_partner(k, carry):
            p_send[n % 2, k] = partial(at_chip(k) * 2 + 1 - core)
            return carry

        def for_own(k, carry):
            own[n % OWN_SLOTS, k] = partial(at_chip(k) * 2 + core)
            return carry

        lax.fori_loop(0, num_chips, for_partner, 0)
        p_copy(n).start()
        lax.fori_loop(0, num_chips, for_own, 0)

    def send_halves(n):
        s = n % OWN_SLOTS
        p_copy(n).wait_recv()
        own[s, 2] = own[s, 2] + p_recv[n, 2]
        for d in (0, 1):
            h_copy(n, d).start()
        for k in (0, 1, 3):
            own[s, k] = own[s, k] + p_recv[n, k]

    def send_full(n):
        s = n % OWN_SLOTS
        for d, k, rng in ((0, 1, low), (1, 3, high)):
            h_copy(n, d).wait_recv()
            own[s, k, rng, :] = own[s, k, rng, :] + h_recv[n, d]
            f_copy(n, d).start()

    def finish(n):
        s = n % OWN_SLOTS
        for d in (0, 1):
            f_copy(n, d).wait_recv()
        out[:, n * nw : (n + 1) * nw] = (own[s, 0] + (f_recv[n, 0] + f_recv[n, 1])).astype(BF16)

    for n in range(OUT_CHUNKS + 2):
        if n < OUT_CHUNKS:
            produce(n)
            send_halves(n)
        if 1 <= n <= OUT_CHUNKS:
            send_full(n - 1)
        if n >= 2:
            finish(n - 2)

    for k in range(1, num_dev):
        plan_copy(k, s_loc, s_all, s_send, s_recv).wait_send()
        plan_copy(k, g_loc, g_all, g_send, g_recv).wait_send()
    for i in range(IN_CHUNKS):
        for kind in range(len(ag_table)):
            ag(i, kind).wait_send()
    for n in range(OUT_CHUNKS - 2, OUT_CHUNKS):
        p_copy(n).wait_send()
    for n in range(OUT_CHUNKS - OWN_SLOTS, OUT_CHUNKS):
        for d in (0, 1):
            h_copy(n, d).wait_send()
            f_copy(n, d).wait_send()


def solution(mesh):
    num_dev = mesh.shape["ep"]
    row_spec = P(("dp", "ep"), None)
    expert_spec = P("ep", None, None)

    def device_step(tokens, routes, w_router, w_one, w_three, w_two):
        num_tokens, d_model = tokens.shape
        num_experts = w_router.shape[1]
        local_experts, _, d_expert = w_one.shape
        cap = slot_capacity(num_tokens, routes.shape[1], num_experts)
        rows, slots = num_dev * cap, local_experts * cap
        kc, nw = d_model // IN_CHUNKS, d_model // OUT_CHUNKS
        chips, half = num_dev // 2, num_tokens // 2
        dma = pltpu.SemaphoreType.DMA
        any_spec = pl.BlockSpec(memory_space=pl.ANY)
        vmem_spec = pl.BlockSpec(memory_space=pltpu.VMEM)
        return pl.pallas_call(
            functools.partial(moe_kernel, cap),
            out_shape=jax.ShapeDtypeStruct((num_tokens, d_model), BF16),
            in_specs=[any_spec, vmem_spec, vmem_spec, any_spec, any_spec, any_spec],
            out_specs=vmem_spec,
            scratch_shapes=[
                pltpu.VMEM((IN_CHUNKS, num_dev, num_tokens, kc), BF16),
                pltpu.VMEM((local_experts, rows, kc), F32),
                pltpu.VMEM((local_experts, rows, d_expert), F32),
                pltpu.VMEM((local_experts, rows, d_expert), F32),
                pltpu.VMEM((local_experts, rows, d_expert), BF16),
                pltpu.VMEM((W_SLOTS, kc, d_expert), BF16),
                pltpu.VMEM((W_SLOTS, kc, d_expert), BF16),
                pltpu.VMEM((2, local_experts, d_expert, nw), BF16),
                pltpu.VMEM((local_experts, rows, nw), F32),
                pltpu.VMEM((num_dev, slots, num_tokens), BF16),
                pltpu.VMEM((num_dev, 3, num_tokens, slots), BF16),
                pltpu.VMEM((num_dev, local_experts, num_tokens), F32),
                pltpu.VMEM((num_dev, local_experts, num_tokens), F32),
                pltpu.VMEM((num_dev, local_experts, num_tokens), F32),
                pltpu.VMEM((num_dev, local_experts, num_tokens), F32),
                pltpu.VMEM((OWN_SLOTS, chips, num_tokens, nw), F32),
                pltpu.VMEM((2, chips, num_tokens, nw), F32),
                pltpu.VMEM((OUT_CHUNKS, chips, num_tokens, nw), F32),
                pltpu.VMEM((OUT_CHUNKS, 2, half, nw), F32),
                pltpu.VMEM((OUT_CHUNKS, 2, num_tokens, nw), F32),
                dma((IN_CHUNKS,)), dma((W_SLOTS,)), dma((W_SLOTS,)), dma((2,)),
                dma((IN_CHUNKS, 9)), dma((IN_CHUNKS, 9)),
                dma((num_dev - 1,)), dma((num_dev - 1,)), dma((num_dev - 1,)), dma((num_dev - 1,)),
                dma((OUT_CHUNKS,)), dma((OUT_CHUNKS,)),
                dma((OUT_CHUNKS, 2)), dma((OUT_CHUNKS, 2)),
                dma((OUT_CHUNKS, 2)), dma((OUT_CHUNKS, 2)),
            ],
            compiler_params=pltpu.CompilerParams(
                collective_id=0, has_side_effects=True, vmem_limit_bytes=67_000_000
            ),
            name="moe_step",
        )(tokens, routes, w_router, w_one, w_three, w_two)

    return jax.shard_map(
        device_step, mesh=mesh,
        in_specs=(row_spec, row_spec, P(None, None), expert_spec, expert_spec, expert_spec),
        out_specs=row_spec, check_vma=False,
    )
```

```python
import functools

import jax
import jax.numpy as jnp
from jax import lax
from jax.experimental import pallas as pl
from jax.experimental.pallas import tpu as pltpu
from jax.sharding import PartitionSpec as P

MESH = pl.DeviceIdType.MESH
F32 = jnp.float32
BF16 = jnp.bfloat16

IN_SPLIT = (1, 2, 2, 2, 1)
OUT_SPLIT = (2, 2, 2, 2, 2, 2, 2, 2)
RING = 24
OWN_SLOTS = 4
FIN_LAG = 3
COLS = 256
EXP_GROUP = 4
GATHER_UNROLL = 4


def chunk_list(parts, total):
    unit = total // sum(parts)
    chunks, at = [], 0
    for part in parts:
        chunks.append((at, part * unit))
        at += part * unit
    return chunks


def slot_capacity(num_tokens, top_k, num_experts):
    return 8 * ((3 * num_tokens * top_k + 16 * num_experts - 1) // (16 * num_experts))


def loop(count, body, unroll):
    if unroll >= count:
        for t in range(count):
            body(t)
        return

    def step(t, carry):
        for r in range(unroll):
            body(t * unroll + r)
        return carry

    lax.fori_loop(0, count // unroll, step, 0)


def moe_kernel(
    cap, tokens, routes, w_router, w_one, w_three, w_two, out,
    xs, us, acc_a, acc_b, hid, pool, y_buf, pick, gate_mat,
    s_loc, g_loc, s_all, g_all, own, p_send, p_recv, h_recv, f_recv,
    tok_sem, in_sem, out_sem, ag_send, ag_recv, s_send, s_recv, g_send, g_recv,
    ps_sem, pr_sem, rs_send, hr_sem, fr_sem, y_sem,
):
    num_tokens, d_model = tokens.shape
    top_k = routes.shape[0]
    num_experts = w_router.shape[0]
    local_experts = w_one.shape[0]
    d_expert = w_one.shape[2]
    num_dev = num_experts // local_experts
    num_chips = num_dev // 2
    ins = chunk_list(IN_SPLIT, d_model)
    outs = chunk_list(OUT_SPLIT, d_model)
    num_in, num_out = len(ins), len(outs)
    unit = d_model // sum(IN_SPLIT)
    rows = num_dev * cap
    slots = local_experts * cap
    half = num_tokens // 2

    me = lax.axis_index("ep")
    chip = me // 2
    core = lax.rem(me, 2)

    def at_chip(k):
        return lax.rem(chip + k, num_chips)

    right = at_chip(1) * 2 + core
    left = at_chip(num_chips - 1) * 2 + core
    opp = at_chip(2) * 2 + core
    partner = chip * 2 + 1 - core

    tiles = d_expert // COLS
    unit_rows = 2 * tiles * unit
    pieces, in_at, out_at, at = [], {}, {}, 0
    for i in range(num_in):
        for e in range(local_experts):
            in_at[i, e] = at
            pieces.append((at, ins[i][1] // unit, i, e))
            at += ins[i][1] // unit
    out_units = local_experts * d_expert // unit_rows
    for n in range(num_out):
        out_at[n] = at
        pieces.append((at, out_units, None, n))
        at += out_units
    started = [0]

    def in_rows(i, e, w, t):
        first = (in_at[i, e] % RING) * unit_rows + (w * tiles + t) * ins[i][1]
        return slice(first, first + ins[i][1])

    def out_rows(n, e):
        first = (out_at[n] % RING) * unit_rows + e * d_expert
        return slice(first, first + d_expert)

    def in_group(i, lo):
        return i * (local_experts // EXP_GROUP) + lo // EXP_GROUP

    def fill(used):
        while started[0] < len(pieces):
            at, units, i, k = pieces[started[0]]
            if at + units > used + RING:
                break
            if i is None:
                for e in range(local_experts):
                    pltpu.make_async_copy(
                        w_two.at[e, :, pl.ds(*outs[k])],
                        pool.at[out_rows(k, e), 0 : outs[k][1]], out_sem.at[k],
                    ).start()
            else:
                for w, ref in enumerate((w_one, w_three)):
                    for t in range(tiles):
                        pltpu.make_async_copy(
                            ref.at[k, pl.ds(*ins[i]), pl.ds(t * COLS, COLS)],
                            pool.at[in_rows(i, k, w, t), :], in_sem.at[in_group(i, k)],
                        ).start()
            started[0] += 1

    def in_wait(i, lo):
        first = (in_at[i, lo] % RING) * unit_rows
        ref = pool.at[first : first + EXP_GROUP * 2 * tiles * ins[i][1], :]
        pltpu.make_async_copy(ref, ref, in_sem.at[in_group(i, lo)]).wait()

    def out_wait(n):
        first = (out_at[n] % RING) * unit_rows
        ref = pool.at[first : first + local_experts * d_expert, 0 : outs[n][1]]
        pltpu.make_async_copy(ref, ref, out_sem.at[n]).wait()

    def tok_copy():
        return pltpu.make_async_copy(tokens, xs.at[me], tok_sem)

    tok_copy().start()

    barrier = pltpu.get_barrier_semaphore()
    for k in range(1, num_dev):
        pl.semaphore_signal(
            barrier, inc=1, device_id={"ep": lax.rem(me + k, num_dev)}, device_id_type=MESH
        )

    expert_id = lax.broadcasted_iota(jnp.int32, (num_experts, num_tokens), 0)
    member = jnp.zeros((num_experts, num_tokens), F32)
    for j in range(top_k):
        member = member + jnp.where(routes[j : j + 1, :] == expert_id, 1.0, 0.0)
    row_id = lax.broadcasted_iota(jnp.int32, (num_tokens, num_tokens), 0)
    col_id = lax.broadcasted_iota(jnp.int32, (num_tokens, num_tokens), 1)
    before = jnp.where(row_id < col_id, 1.0, 0.0).astype(BF16)
    rank = jnp.dot(member.astype(BF16), before, preferred_element_type=F32)
    slot_of = jnp.where(member > 0.5, rank, -1.0)
    s_loc[...] = slot_of.reshape(num_dev, local_experts, num_tokens)
    s_all[me] = s_loc[me]

    with jax.named_scope("tok_wait"):
        tok_copy().wait()
    fill(0)

    with jax.named_scope("barrier"):
        pl.semaphore_wait(barrier, num_dev - 1)

    def plan_copy(k, src, dst, send, recv):
        peer = lax.rem(me + k, num_dev)
        return pltpu.make_async_remote_copy(
            src_ref=src.at[peer], dst_ref=dst.at[me], send_sem=send, recv_sem=recv,
            device_id={"ep": peer}, device_id_type=MESH,
        )

    def plan_all(src, dst, send, recv):
        return pltpu.make_async_remote_copy(
            src_ref=src.at[0 : num_dev - 1], dst_ref=dst.at[0 : num_dev - 1], send_sem=send,
            recv_sem=recv, device_id={"ep": partner}, device_id_type=MESH,
        )

    for k in range(1, num_dev):
        plan_copy(k, s_loc, s_all, s_send, s_recv).start()

    low, high, full = pl.ds(0, half), pl.ds(half, half), pl.ds(0, num_tokens)
    ag_table = (
        (me, full, right), (me, full, left), (me, full, partner),
        (left, low, right), (right, high, left),
        (left, full, partner), (right, full, partner),
        (opp, low, partner), (opp, high, partner),
    )

    ag_sem = (0, 1, 4, 2, 3, 4, 4, 4, 4)

    def ag(i, kind):
        block, rng, dest = ag_table[kind]
        ref = xs.at[block, rng, pl.ds(*ins[i])]
        return pltpu.make_async_remote_copy(
            src_ref=ref, dst_ref=ref, send_sem=ag_send,
            recv_sem=ag_recv.at[i, ag_sem[kind]], device_id={"ep": dest}, device_id_type=MESH,
        )

    def ag_partner(i):
        ref = xs.at[0 : num_dev // 2, :, pl.ds(*ins[i])]
        return pltpu.make_async_remote_copy(
            src_ref=ref, dst_ref=ref, send_sem=ag_send,
            recv_sem=ag_recv.at[i, 4], device_id={"ep": partner}, device_id_type=MESH,
        )

    def ag_own(i):
        if i < num_in:
            for kind in (0, 1, 2):
                ag(i, kind).start()

    def ag_stage1(i):
        if i < num_in:
            ag(i, 0).wait_recv()
            ag(i, 3).start()
            ag(i, 5).start()
            ag(i, 1).wait_recv()
            ag(i, 4).start()
            ag(i, 6).start()
            ag_own(i + 2)

    def ag_stage2(i):
        if i < num_in:
            ag(i, 3).wait_recv()
            ag(i, 7).start()
            ag(i, 4).wait_recv()
            ag(i, 8).start()

    def ag_stage3(i):
        if i < num_in:
            ag_partner(i).wait_recv()

    ag_own(0)

    def span(i):
        return ins[i][0], ins[i][0] + ins[i][1]

    dims = (((1,), (1,)), ((), ()))
    logits = jnp.zeros((num_experts, num_tokens), F32)
    for i in range(num_in):
        logits = logits + lax.dot_general(
            w_router[:, slice(*span(i))], xs[me, :, slice(*span(i))], dims, preferred_element_type=F32
        )
    chosen = member > 0.5
    peak = jnp.max(jnp.where(chosen, logits, -jnp.inf), axis=0, keepdims=True)
    powers = jnp.where(chosen, jnp.exp(jnp.where(chosen, logits - peak, 0.0)), 0.0)
    gates = powers / jnp.sum(powers, axis=0, keepdims=True)
    g_loc[...] = gates.reshape(num_dev, local_experts, num_tokens)
    g_all[me] = g_loc[me]
    for k in range(1, num_dev):
        plan_copy(k, g_loc, g_all, g_send, g_recv).start()
    ag_own(1)

    slot_id = lax.broadcasted_iota(jnp.int32, (cap, num_tokens), 0).astype(F32)
    with jax.named_scope("s_wait"):
        plan_all(s_loc, s_all, s_send, s_recv).wait_recv()

    def build_pick(q, carry):
        parts = [
            jnp.where(s_all[q, e : e + 1, :] == slot_id, 1.0, 0.0) for e in range(local_experts)
        ]
        pick[q] = jnp.concatenate(parts, axis=0).astype(BF16)
        return carry

    with jax.named_scope("build_pick"):
        lax.fori_loop(0, num_dev, build_pick, 0)

    def build_gates(q, carry):
        parts = [
            jnp.where(s_all[q, e : e + 1, :] == slot_id, g_all[q, e : e + 1, :], 0.0)
            for e in range(local_experts)
        ]
        mat = jnp.concatenate(parts, axis=0).T
        top = mat.astype(BF16)
        rest = mat - top.astype(F32)
        mid = rest.astype(BF16)
        gate_mat[q, 0:num_tokens] = top
        gate_mat[q, num_tokens : 2 * num_tokens] = mid
        gate_mat[q, 2 * num_tokens :] = (rest - mid.astype(F32)).astype(BF16)
        return carry

    def gather(i):
        def one_source(q):
            width = ins[i][1]
            picked = jnp.dot(pick[q], xs[q, :, slice(*span(i))], preferred_element_type=F32)
            us[:, pl.ds(q * cap, cap), 0:width] = picked.reshape(local_experts, cap, width)

        loop(num_dev, one_source, GATHER_UNROLL)

    def experts(i, first, last):
        for lo in range(first, last, EXP_GROUP):
            expert_group(i, lo, lo + EXP_GROUP)

    def expert_group(i, lo, hi):
        in_wait(i, lo)
        for e in range(lo, hi):
            u = us[e, :, 0 : ins[i][1]].astype(BF16)
            for t in range(tiles):
                cols = slice(t * COLS, (t + 1) * COLS)
                a = jnp.dot(u, pool[in_rows(i, e, 0, t), :], preferred_element_type=F32)
                b = jnp.dot(u, pool[in_rows(i, e, 1, t), :], preferred_element_type=F32)
                if i > 0:
                    a = a + acc_a[e, :, cols]
                    b = b + acc_b[e, :, cols]
                if i < num_in - 1:
                    acc_a[e, :, cols] = a
                    acc_b[e, :, cols] = b
                else:
                    hid[e, :, cols] = (jax.nn.silu(a) * b).astype(BF16)
        fill(in_at[i, hi - 1] + ins[i][1] // unit)

    with jax.named_scope("ag1_0"):
        ag_stage1(0)
    with jax.named_scope("g_wait"):
        plan_all(g_loc, g_all, g_send, g_recv).wait_recv()
    with jax.named_scope("build_gates"):
        lax.fori_loop(0, num_dev, build_gates, 0)
    with jax.named_scope("ag2_0"):
        ag_stage2(0)
    with jax.named_scope("ag1_1"):
        ag_stage1(1)
    with jax.named_scope("ag3_0"):
        ag_stage3(0)
    mid_expert = local_experts // 2
    for i in range(num_in):
        with jax.named_scope(f"gather_{i}"):
            gather(i)
        with jax.named_scope(f"experts_{i}a"):
            experts(i, 0, mid_expert)
        with jax.named_scope(f"ag1_{i + 2}"):
            ag_stage1(i + 2)
        with jax.named_scope(f"ag2_{i + 1}"):
            ag_stage2(i + 1)
        with jax.named_scope(f"experts_{i}b"):
            experts(i, mid_expert, local_experts)
        with jax.named_scope(f"ag3_{i + 1}"):
            ag_stage3(i + 1)

    def partial(n, q):
        nw = outs[n][1]
        base = pl.multiple_of(q * cap, 8)
        o_rows = us[:, pl.ds(base, cap), 0:nw].reshape(slots, nw).astype(BF16)
        total = jnp.dot(gate_mat[q], o_rows, preferred_element_type=F32)
        total = total.reshape(3, num_tokens, nw)
        return (total[2] + total[1]) + total[0]

    def width(n):
        return pl.ds(0, outs[n][1])

    order = (2, 1, 3, 0)

    def p_copy(n, part):
        js = slice(0, 1) if part == 0 else slice(1, num_chips)
        return pltpu.make_async_remote_copy(
            src_ref=p_send.at[n % 2, js, :, width(n)], dst_ref=p_recv.at[n, js, :, width(n)],
            send_sem=ps_sem.at[n % 2], recv_sem=pr_sem.at[n, part],
            device_id={"ep": partner}, device_id_type=MESH,
        )

    def p_sent(n):
        pltpu.make_async_remote_copy(
            src_ref=p_send.at[n % 2, :, :, width(n)], dst_ref=p_recv.at[n, :, :, width(n)],
            send_sem=ps_sem.at[n % 2], recv_sem=pr_sem.at[n, 0],
            device_id={"ep": partner}, device_id_type=MESH,
        ).wait_send()

    def h_copy(n, d):
        return pltpu.make_async_remote_copy(
            src_ref=own.at[n % OWN_SLOTS, 2, low if d == 0 else high, width(n)],
            dst_ref=h_recv.at[n, d, :, width(n)], send_sem=rs_send.at[n % OWN_SLOTS],
            recv_sem=hr_sem.at[n, d],
            device_id={"ep": right if d == 0 else left}, device_id_type=MESH,
        )

    def f_copy(n, d):
        return pltpu.make_async_remote_copy(
            src_ref=own.at[n % OWN_SLOTS, 1 if d == 0 else 3, :, width(n)],
            dst_ref=f_recv.at[n, d, :, width(n)], send_sem=rs_send.at[n % OWN_SLOTS],
            recv_sem=fr_sem.at[n],
            device_id={"ep": right if d == 0 else left}, device_id_type=MESH,
        )

    def ring_sent(n):
        ref = own.at[n % OWN_SLOTS, 0:3, :, width(n)]
        pltpu.make_async_remote_copy(
            src_ref=ref, dst_ref=ref, send_sem=rs_send.at[n % OWN_SLOTS], recv_sem=fr_sem.at[n],
            device_id={"ep": right}, device_id_type=MESH,
        ).wait_send()

    def down(n):
        out_wait(n)
        w = slice(0, outs[n][1])
        for e in range(local_experts):
            us[e, :, w] = jnp.dot(hid[e], pool[out_rows(n, e), w], preferred_element_type=F32)

    def combine(n):
        w = slice(0, outs[n][1])
        if n >= 2:
            p_sent(n - 2)
        if n >= OWN_SLOTS:
            ring_sent(n - OWN_SLOTS)
        for js in ((0,), (1, 2, 3)):
            for j in js:
                p_send[n % 2, j, :, w] = partial(n, at_chip(order[j]) * 2 + 1 - core)
            p_copy(n, js[0]).start() if js[0] == 0 else p_copy(n, 1).start()
            for j in js:
                own[n % OWN_SLOTS, order[j], :, w] = partial(n, at_chip(order[j]) * 2 + core)
        fill(out_at[n] + out_units)

    def send_halves(n):
        s, w = n % OWN_SLOTS, slice(0, outs[n][1])
        p_copy(n, 0).wait_recv()
        own[s, 2, :, w] = own[s, 2, :, w] + p_recv[n, 0, :, w]
        for d in (0, 1):
            h_copy(n, d).start()

    def add_partner(n):
        s, w = n % OWN_SLOTS, slice(0, outs[n][1])
        p_copy(n, 1).wait_recv()
        for j in (1, 2, 3):
            own[s, order[j], :, w] = own[s, order[j], :, w] + p_recv[n, j, :, w]

    def send_full(n):
        s, w = n % OWN_SLOTS, slice(0, outs[n][1])
        for d, k, rng in ((0, 1, low), (1, 3, high)):
            h_copy(n, d).wait_recv()
            own[s, k, rng, w] = own[s, k, rng, w] + h_recv[n, d, :, w]
            f_copy(n, d).start()

    def y_copy(n):
        cols = pl.ds(*outs[n])
        return pltpu.make_async_copy(y_buf.at[:, cols], out.at[:, cols], y_sem)

    def finish(n):
        s, w = n % OWN_SLOTS, slice(0, outs[n][1])
        ref = f_recv.at[n, :, :, width(n)]
        pltpu.make_async_remote_copy(
            src_ref=ref, dst_ref=ref, send_sem=rs_send.at[s], recv_sem=fr_sem.at[n],
            device_id={"ep": right}, device_id_type=MESH,
        ).wait_recv()
        y_buf[:, pl.ds(*outs[n])] = (
            own[s, 0, :, w] + (f_recv[n, 0, :, w] + f_recv[n, 1, :, w])
        ).astype(BF16)
        y_copy(n).start()

    def run(name, body, n, lag=0):
        if 0 <= n - lag < num_out:
            with jax.named_scope(f"{name}_{n - lag}"):
                body(n - lag)

    for n in range(num_out + FIN_LAG):
        run("down", down, n)
        if n >= 2:
            run("halves", send_halves, n, 1)
        run("combine", combine, n)
        if n == 0:
            run("halves", send_halves, n)
        run("add", add_partner, n, 1)
        run("full", send_full, n, 2)
        run("finish", finish, n, FIN_LAG)

    with jax.named_scope("end_plan"):
        plan_all(s_loc, s_all, s_send, s_recv).wait_send()
        plan_all(g_loc, g_all, g_send, g_recv).wait_send()
        sent = xs.at[0 : num_dev - 1]
        pltpu.make_async_remote_copy(
            src_ref=sent, dst_ref=sent, send_sem=ag_send, recv_sem=ag_recv.at[0, 4],
            device_id={"ep": partner}, device_id_type=MESH,
        ).wait_send()
    with jax.named_scope("end_ring"):
        for n in range(num_out - 2, num_out):
            p_sent(n)
        for n in range(num_out - OWN_SLOTS, num_out):
            ring_sent(n)
    with jax.named_scope("end_y"):
        pltpu.make_async_copy(y_buf, out, y_sem).wait()


def solution(mesh):
    num_dev = mesh.shape["ep"]
    row_spec = P(("dp", "ep"), None)
    expert_spec = P("ep", None, None)

    def device_step(tokens, routes, w_router, w_one, w_three, w_two):
        num_tokens, d_model = tokens.shape
        num_experts = w_router.shape[1]
        local_experts, _, d_expert = w_one.shape
        cap = slot_capacity(num_tokens, routes.shape[1], num_experts)
        rows, slots = num_dev * cap, local_experts * cap
        num_in, num_out = len(IN_SPLIT), len(OUT_SPLIT)
        unit = d_model // sum(IN_SPLIT)
        kc = unit * max(IN_SPLIT)
        nw = d_model // sum(OUT_SPLIT) * max(OUT_SPLIT)
        chips, half = num_dev // 2, num_tokens // 2
        dma = pltpu.SemaphoreType.DMA
        any_spec = pl.BlockSpec(memory_space=pl.ANY)
        vmem_spec = pl.BlockSpec(memory_space=pltpu.VMEM)
        return pl.pallas_call(
            functools.partial(moe_kernel, cap),
            out_shape=jax.ShapeDtypeStruct((num_tokens, d_model), BF16),
            in_specs=[any_spec, vmem_spec, vmem_spec, any_spec, any_spec, any_spec],
            out_specs=any_spec,
            scratch_shapes=[
                pltpu.VMEM((num_dev, num_tokens, d_model), BF16),
                pltpu.VMEM((local_experts, rows, kc), F32),
                pltpu.VMEM((local_experts, rows, d_expert), F32),
                pltpu.VMEM((local_experts, rows, d_expert), F32),
                pltpu.VMEM((local_experts, rows, d_expert), BF16),
                pltpu.VMEM((RING * 2 * d_expert // COLS * unit, COLS), BF16),
                pltpu.VMEM((num_tokens, d_model), BF16),
                pltpu.VMEM((num_dev, slots, num_tokens), BF16),
                pltpu.VMEM((num_dev, 3 * num_tokens, slots), BF16),
                pltpu.VMEM((num_dev, local_experts, num_tokens), F32),
                pltpu.VMEM((num_dev, local_experts, num_tokens), F32),
                pltpu.VMEM((num_dev, local_experts, num_tokens), F32),
                pltpu.VMEM((num_dev, local_experts, num_tokens), F32),
                pltpu.VMEM((OWN_SLOTS, chips, num_tokens, nw), F32),
                pltpu.VMEM((2, chips, num_tokens, nw), F32),
                pltpu.VMEM((num_out, chips, num_tokens, nw), F32),
                pltpu.VMEM((num_out, 2, half, nw), F32),
                pltpu.VMEM((num_out, 2, num_tokens, nw), F32),
                dma, dma((num_in * local_experts // EXP_GROUP,)), dma((num_out,)),
                dma, dma((num_in, 5)), dma, dma, dma, dma,
                dma((2,)), dma((num_out, 2)), dma((OWN_SLOTS,)), dma((num_out, 2)), dma((num_out,)), dma,
            ],
            compiler_params=pltpu.CompilerParams(
                collective_id=0, has_side_effects=True, vmem_limit_bytes=67_000_000
            ),
            name="moe_step",
        )(tokens, routes.T, w_router.T, w_one, w_three, w_two)

    return jax.shard_map(
        device_step, mesh=mesh,
        in_specs=(row_spec, row_spec, P(None, None), expert_spec, expert_spec, expert_spec),
        out_specs=row_spec, check_vma=False,
    )
```

```python
import functools

import jax
import jax.numpy as jnp
from jax import lax
from jax.experimental import pallas as pl
from jax.experimental.pallas import tpu as pltpu
from jax.sharding import PartitionSpec as P

MESH = pl.DeviceIdType.MESH
F32 = jnp.float32
BF16 = jnp.bfloat16

IN_SPLIT = (1, 2, 2, 2, 1)
AG_START = ("s", "f0", "o2", "g", "f1", "o3", "h0", "p0")
AG_PLAN = (((), (), ("f2", "h1", "p1")), (("o4",), ("f3", "h2"), ("p2",)), ((), ("f4", "h3"), ("p3",)), ((), ("h4",), ("p4",)), ((), (), ()))
OUT_SPLIT = (2, 2, 2, 2, 2, 2, 2, 2)
RING = 24
OWN_SLOTS = 4
FIN_LAG = 3
EARLY = 2
FULL_EARLY = 1
COLS = 256
EXP_GROUP = 4
GATHER_UNROLL = 8


def chunk_list(parts, total):
    unit = total // sum(parts)
    chunks, at = [], 0
    for part in parts:
        chunks.append((at, part * unit))
        at += part * unit
    return chunks


def slot_capacity(num_tokens, top_k, num_experts):
    return 8 * ((3 * num_tokens * top_k + 16 * num_experts - 1) // (16 * num_experts))


def loop(count, body, unroll):
    if unroll >= count:
        for t in range(count):
            body(t)
        return

    def step(t, carry):
        for r in range(unroll):
            body(t * unroll + r)
        return carry

    lax.fori_loop(0, count // unroll, step, 0)


def moe_kernel(
    cap, tokens, routes_in, w_router_in, w_one, w_three, w_two, out,
    routes, w_router, xs, us, acc_a, acc_b, hid, pool, pick, gate_mat,
    s_loc, g_loc, s_all, g_all, own, p_send, p_recv, h_recv, f_recv,
    tok_sem, route_sem, router_sem, in_sem, out_sem, ag_send, ag_recv, s_send, s_recv, g_send, g_recv,
    ps_sem, pr_sem, rs_send, hr_sem, fr_sem,
):
    num_tokens, d_model = tokens.shape
    top_k = routes.shape[0]
    num_experts = w_router.shape[0]
    local_experts = w_one.shape[0]
    d_expert = w_one.shape[2]
    num_dev = num_experts // local_experts
    num_chips = num_dev // 2
    ins = chunk_list(IN_SPLIT, d_model)
    outs = chunk_list(OUT_SPLIT, d_model)
    num_in, num_out = len(ins), len(outs)
    unit = d_model // sum(IN_SPLIT)
    rows = num_dev * cap
    slots = local_experts * cap
    half = num_tokens // 2

    me = lax.axis_index("ep")
    chip = me // 2
    core = lax.rem(me, 2)

    def at_chip(k):
        return lax.rem(chip + k, num_chips)

    right = at_chip(1) * 2 + core
    left = at_chip(num_chips - 1) * 2 + core
    opp = at_chip(2) * 2 + core
    partner = chip * 2 + 1 - core

    tiles = d_expert // COLS
    unit_rows = 2 * tiles * unit
    pieces, in_at, out_at, at = [], {}, {}, 0
    for i in range(num_in):
        for e in range(local_experts):
            in_at[i, e] = at
            pieces.append((at, ins[i][1] // unit, i, e))
            at += ins[i][1] // unit
    out_units = local_experts * d_expert // unit_rows
    for n in range(num_out):
        out_at[n] = at
        pieces.append((at, out_units, None, n))
        at += out_units
    started = [0]

    def in_rows(i, e, w, t):
        first = (in_at[i, e] % RING) * unit_rows + (w * tiles + t) * ins[i][1]
        return slice(first, first + ins[i][1])

    def out_rows(n, e):
        first = (out_at[n] % RING) * unit_rows + e * d_expert
        return slice(first, first + d_expert)

    def in_group(i, lo):
        return i * (local_experts // EXP_GROUP) + lo // EXP_GROUP

    def fill(used):
        while started[0] < len(pieces):
            at, units, i, k = pieces[started[0]]
            if at + units > used + RING:
                break
            if i is None:
                for e in range(local_experts):
                    pltpu.make_async_copy(
                        w_two.at[e, :, pl.ds(*outs[k])],
                        pool.at[out_rows(k, e), 0 : outs[k][1]], out_sem.at[k],
                    ).start()
            else:
                for w, ref in enumerate((w_one, w_three)):
                    for t in range(tiles):
                        pltpu.make_async_copy(
                            ref.at[k, pl.ds(*ins[i]), pl.ds(t * COLS, COLS)],
                            pool.at[in_rows(i, k, w, t), :], in_sem.at[in_group(i, k)],
                        ).start()
            started[0] += 1

    def in_wait(i, lo):
        first = (in_at[i, lo] % RING) * unit_rows
        ref = pool.at[first : first + EXP_GROUP * 2 * tiles * ins[i][1], :]
        pltpu.make_async_copy(ref, ref, in_sem.at[in_group(i, lo)]).wait()

    def out_wait(n):
        first = (out_at[n] % RING) * unit_rows
        ref = pool.at[first : first + local_experts * d_expert, 0 : outs[n][1]]
        pltpu.make_async_copy(ref, ref, out_sem.at[n]).wait()

    def tok_copy():
        return pltpu.make_async_copy(tokens, xs.at[me], tok_sem)

    route_copy = pltpu.make_async_copy(routes_in, routes, route_sem)
    router_copy = pltpu.make_async_copy(w_router_in, w_router, router_sem)
    tok_copy().start()
    route_copy.start()
    router_copy.start()

    barrier = pltpu.get_barrier_semaphore()
    for k in range(1, num_dev):
        pl.semaphore_signal(
            barrier, inc=1, device_id={"ep": lax.rem(me + k, num_dev)}, device_id_type=MESH
        )

    with jax.named_scope("tok_wait"):
        tok_copy().wait()
    fill(0)

    with jax.named_scope("barrier"):
        pl.semaphore_wait(barrier, num_dev - 1)

    low, high, full = pl.ds(0, half), pl.ds(half, half), pl.ds(0, num_tokens)
    ag_table = (
        (me, full, right), (me, full, left), (me, full, partner),
        (left, low, right), (right, high, left),
        (left, full, partner), (right, full, partner),
        (opp, low, partner), (opp, high, partner),
    )

    ag_sem = (0, 1, 4, 2, 3, 4, 4, 4, 4)

    def ag(i, kind):
        block, rng, dest = ag_table[kind]
        ref = xs.at[block, rng, pl.ds(*ins[i])]
        return pltpu.make_async_remote_copy(
            src_ref=ref, dst_ref=ref, send_sem=ag_send,
            recv_sem=ag_recv.at[i, ag_sem[kind]], device_id={"ep": dest}, device_id_type=MESH,
        )

    def ag_partner(i):
        ref = xs.at[0 : num_dev // 2, :, pl.ds(*ins[i])]
        return pltpu.make_async_remote_copy(
            src_ref=ref, dst_ref=ref, send_sem=ag_send,
            recv_sem=ag_recv.at[i, 4], device_id={"ep": partner}, device_id_type=MESH,
        )

    def ag_own(i):
        if i < num_in:
            for kind in (0, 1, 2):
                ag(i, kind).start()

    def ag_stage1(i):
        if i < num_in:
            ag(i, 0).wait_recv()
            ag(i, 3).start()
            ag(i, 5).start()
            ag(i, 1).wait_recv()
            ag(i, 4).start()
            ag(i, 6).start()

    def ag_stage2(i):
        if i < num_in:
            ag(i, 3).wait_recv()
            ag(i, 7).start()
            ag(i, 4).wait_recv()
            ag(i, 8).start()

    def ag_stage3(i):
        if i < num_in:
            ag_partner(i).wait_recv()

    ag_own(0)

    route_copy.wait()
    expert_id = lax.broadcasted_iota(jnp.int32, (num_experts, num_tokens), 0)
    member = jnp.zeros((num_experts, num_tokens), F32)
    for j in range(top_k):
        member = member + jnp.where(routes[j : j + 1, :] == expert_id, 1.0, 0.0)
    row_id = lax.broadcasted_iota(jnp.int32, (num_tokens, num_tokens), 0)
    col_id = lax.broadcasted_iota(jnp.int32, (num_tokens, num_tokens), 1)
    before = jnp.where(row_id < col_id, 1.0, 0.0).astype(BF16)
    rank = jnp.dot(member.astype(BF16), before, preferred_element_type=F32)
    slot_of = jnp.where(member > 0.5, rank, -1.0)
    s_loc[...] = slot_of.reshape(num_dev, local_experts, num_tokens)
    s_all[me] = s_loc[me]

    def plan_copy(k, src, dst, send, recv):
        peer = lax.rem(me + k, num_dev)
        return pltpu.make_async_remote_copy(
            src_ref=src.at[peer], dst_ref=dst.at[me], send_sem=send, recv_sem=recv,
            device_id={"ep": peer}, device_id_type=MESH,
        )

    def plan_all(src, dst, send, recv):
        return pltpu.make_async_remote_copy(
            src_ref=src.at[0 : num_dev - 1], dst_ref=dst.at[0 : num_dev - 1], send_sem=send,
            recv_sem=recv, device_id={"ep": partner}, device_id_type=MESH,
        )

    for k in range(1, num_dev):
        plan_copy(k, s_loc, s_all, s_send, s_recv).start()

    def span(i):
        return ins[i][0], ins[i][0] + ins[i][1]

    dims = (((1,), (1,)), ((), ()))
    logits = jnp.zeros((num_experts, num_tokens), F32)
    router_copy.wait()
    for i in range(num_in):
        logits = logits + lax.dot_general(
            w_router[:, slice(*span(i))], xs[me, :, slice(*span(i))], dims, preferred_element_type=F32
        )
    chosen = member > 0.5
    peak = jnp.max(jnp.where(chosen, logits, -jnp.inf), axis=0, keepdims=True)
    powers = jnp.where(chosen, jnp.exp(jnp.where(chosen, logits - peak, 0.0)), 0.0)
    gates = powers / jnp.sum(powers, axis=0, keepdims=True)
    g_loc[...] = gates.reshape(num_dev, local_experts, num_tokens)
    g_all[me] = g_loc[me]
    for k in range(1, num_dev):
        plan_copy(k, g_loc, g_all, g_send, g_recv).start()
    ag_own(1)

    slot_id = lax.broadcasted_iota(jnp.int32, (cap, num_tokens), 0).astype(F32)
    def build_pick(q, carry):
        parts = [
            jnp.where(s_all[q, e : e + 1, :] == slot_id, 1.0, 0.0) for e in range(local_experts)
        ]
        pick[q] = jnp.concatenate(parts, axis=0).astype(BF16)
        return carry


    def build_gates(q, carry):
        parts = [
            jnp.where(s_all[q, e : e + 1, :] == slot_id, g_all[q, e : e + 1, :], 0.0)
            for e in range(local_experts)
        ]
        mat = jnp.concatenate(parts, axis=0).T
        top = mat.astype(BF16)
        rest = mat - top.astype(F32)
        mid = rest.astype(BF16)
        gate_mat[q, 0:num_tokens] = top
        gate_mat[q, num_tokens : 2 * num_tokens] = mid
        gate_mat[q, 2 * num_tokens :] = (rest - mid.astype(F32)).astype(BF16)
        return carry

    def gather(i):
        def one_source(q):
            width = ins[i][1]
            picked = jnp.dot(pick[q], xs[q, :, slice(*span(i))], preferred_element_type=F32)
            us[:, pl.ds(q * cap, cap), 0:width] = picked.reshape(local_experts, cap, width)

        if GATHER_UNROLL < num_dev:
            loop(num_dev, one_source, GATHER_UNROLL)
        else:

            @pl.when(me >= 0)
            def _():
                loop(num_dev, one_source, num_dev)

    def experts(i, first, last):
        for lo in range(first, last, EXP_GROUP):
            expert_group(i, lo, lo + EXP_GROUP)

    def expert_group(i, lo, hi):
        in_wait(i, lo)
        for e in range(lo, hi):
            u = us[e, :, 0 : ins[i][1]].astype(BF16)
            for t in range(tiles):
                cols = slice(t * COLS, (t + 1) * COLS)
                a = jnp.dot(u, pool[in_rows(i, e, 0, t), :], preferred_element_type=F32)
                b = jnp.dot(u, pool[in_rows(i, e, 1, t), :], preferred_element_type=F32)
                if i > 0:
                    a = a + acc_a[e, :, cols]
                    b = b + acc_b[e, :, cols]
                if i < num_in - 1:
                    acc_a[e, :, cols] = a
                    acc_b[e, :, cols] = b
                else:
                    hid[e, :, cols] = (jax.nn.silu(a) * b).astype(BF16)
        fill(in_at[i, hi - 1] + ins[i][1] // unit)

    def slots_ready():
        plan_all(s_loc, s_all, s_send, s_recv).wait_recv()
        lax.fori_loop(0, num_dev, build_pick, 0)

    def gates_ready():
        plan_all(g_loc, g_all, g_send, g_recv).wait_recv()
        lax.fori_loop(0, num_dev, build_gates, 0)

    plans = {"s": slots_ready, "g": gates_ready}
    actions = {"f": ag_stage1, "h": ag_stage2, "p": ag_stage3, "o": ag_own}

    def hook(items):
        for item in items:
            with jax.named_scope("ag_" + item):
                actions[item[0]](int(item[1:])) if item[1:] else plans[item]()

    hook(AG_START)
    mid_expert = local_experts // 2
    for i in range(num_in):
        with jax.named_scope(f"gather_{i}"):
            gather(i)
        hook(AG_PLAN[i][0])
        with jax.named_scope(f"experts_{i}a"):
            experts(i, 0, mid_expert)
        hook(AG_PLAN[i][1])
        with jax.named_scope(f"experts_{i}b"):
            experts(i, mid_expert, local_experts)
        hook(AG_PLAN[i][2])

    def partial(n, q):
        nw = outs[n][1]
        base = pl.multiple_of(q * cap, 8)
        o_rows = us[:, pl.ds(base, cap), 0:nw].reshape(slots, nw).astype(BF16)
        total = jnp.dot(gate_mat[q], o_rows, preferred_element_type=F32)
        total = total.reshape(3, num_tokens, nw)
        return (total[2] + total[1]) + total[0]

    def width(n):
        return pl.ds(0, outs[n][1])

    order = (2, 1, 3, 0)

    def p_copy(n, part):
        js = slice(0, 1) if part == 0 else slice(1, num_chips)
        return pltpu.make_async_remote_copy(
            src_ref=p_send.at[n % 2, js, :, width(n)], dst_ref=p_recv.at[n, js, :, width(n)],
            send_sem=ps_sem.at[n % 2], recv_sem=pr_sem.at[n, part],
            device_id={"ep": partner}, device_id_type=MESH,
        )

    def p_sent(n):
        pltpu.make_async_remote_copy(
            src_ref=p_send.at[n % 2, :, :, width(n)], dst_ref=p_recv.at[n, :, :, width(n)],
            send_sem=ps_sem.at[n % 2], recv_sem=pr_sem.at[n, 0],
            device_id={"ep": partner}, device_id_type=MESH,
        ).wait_send()

    def h_copy(n, d):
        return pltpu.make_async_remote_copy(
            src_ref=own.at[n % OWN_SLOTS, 2, low if d == 0 else high, width(n)],
            dst_ref=h_recv.at[n, d, :, width(n)], send_sem=rs_send.at[n % OWN_SLOTS],
            recv_sem=hr_sem.at[n, d],
            device_id={"ep": right if d == 0 else left}, device_id_type=MESH,
        )

    def f_copy(n, d):
        return pltpu.make_async_remote_copy(
            src_ref=own.at[n % OWN_SLOTS, 1 if d == 0 else 3, :, width(n)],
            dst_ref=f_recv.at[n, d, :, width(n)], send_sem=rs_send.at[n % OWN_SLOTS],
            recv_sem=fr_sem.at[n],
            device_id={"ep": right if d == 0 else left}, device_id_type=MESH,
        )

    def ring_sent(n):
        ref = own.at[n % OWN_SLOTS, 0:3, :, width(n)]
        pltpu.make_async_remote_copy(
            src_ref=ref, dst_ref=ref, send_sem=rs_send.at[n % OWN_SLOTS], recv_sem=fr_sem.at[n],
            device_id={"ep": right}, device_id_type=MESH,
        ).wait_send()

    def down(n):
        out_wait(n)
        w = slice(0, outs[n][1])
        for e in range(local_experts):
            us[e, :, w] = jnp.dot(hid[e], pool[out_rows(n, e), w], preferred_element_type=F32)

    def combine(n):
        w = slice(0, outs[n][1])
        if n >= 2:
            p_sent(n - 2)
        if n >= OWN_SLOTS:
            ring_sent(n - OWN_SLOTS)
        for part, js in enumerate(((0,), (1, 2, 3))):
            for j in js:
                p_send[n % 2, j, :, w] = partial(n, at_chip(order[j]) * 2 + 1 - core)
            p_copy(n, part).start()
        for j in range(num_chips):
            own[n % OWN_SLOTS, order[j], :, w] = partial(n, at_chip(order[j]) * 2 + core)
        fill(out_at[n] + out_units)

    def send_halves(n):
        s, w = n % OWN_SLOTS, slice(0, outs[n][1])
        p_copy(n, 0).wait_recv()
        own[s, 2, :, w] = own[s, 2, :, w] + p_recv[n, 0, :, w]
        for d in (0, 1):
            h_copy(n, d).start()

    def add_partner(n):
        s, w = n % OWN_SLOTS, slice(0, outs[n][1])
        p_copy(n, 1).wait_recv()
        for j in (1, 2, 3):
            own[s, order[j], :, w] = own[s, order[j], :, w] + p_recv[n, j, :, w]

    def send_full(n):
        s, w = n % OWN_SLOTS, slice(0, outs[n][1])
        for d, k, rng in ((0, 1, low), (1, 3, high)):
            h_copy(n, d).wait_recv()
            own[s, k, rng, w] = own[s, k, rng, w] + h_recv[n, d, :, w]
            f_copy(n, d).start()

    def finish(n):
        s, w = n % OWN_SLOTS, slice(0, outs[n][1])
        ref = f_recv.at[n, :, :, width(n)]
        pltpu.make_async_remote_copy(
            src_ref=ref, dst_ref=ref, send_sem=rs_send.at[s], recv_sem=fr_sem.at[n],
            device_id={"ep": right}, device_id_type=MESH,
        ).wait_recv()
        out[:, pl.ds(*outs[n])] = (
            own[s, 0, :, w] + (f_recv[n, 0, :, w] + f_recv[n, 1, :, w])
        ).astype(BF16)

    def run(name, body, n, lag=0):
        if 0 <= n - lag < num_out:
            with jax.named_scope(f"{name}_{n - lag}"):
                body(n - lag)

    for n in range(num_out + FIN_LAG):
        run("down", down, n)
        if n >= 1 + EARLY:
            run("halves", send_halves, n, 1)
        if FULL_EARLY:
            run("add", add_partner, n, 2)
            run("full", send_full, n, 2)
        run("combine", combine, n)
        if n < EARLY:
            run("halves", send_halves, n)
        if not FULL_EARLY:
            run("add", add_partner, n, 1)
            run("full", send_full, n, 2)
        run("finish", finish, n, FIN_LAG)

    with jax.named_scope("end_plan"):
        plan_all(s_loc, s_all, s_send, s_recv).wait_send()
        plan_all(g_loc, g_all, g_send, g_recv).wait_send()
        sent = xs.at[0 : num_dev - 1]
        pltpu.make_async_remote_copy(
            src_ref=sent, dst_ref=sent, send_sem=ag_send, recv_sem=ag_recv.at[0, 4],
            device_id={"ep": partner}, device_id_type=MESH,
        ).wait_send()
    with jax.named_scope("end_ring"):
        for n in range(num_out - 2, num_out):
            p_sent(n)
        for n in range(num_out - OWN_SLOTS, num_out):
            ring_sent(n)


def solution(mesh):
    num_dev = mesh.shape["ep"]
    row_spec = P(("dp", "ep"), None)
    expert_spec = P("ep", None, None)

    def device_step(tokens, routes, w_router, w_one, w_three, w_two):
        num_tokens, d_model = tokens.shape
        num_experts = w_router.shape[1]
        local_experts, _, d_expert = w_one.shape
        cap = slot_capacity(num_tokens, routes.shape[1], num_experts)
        rows, slots = num_dev * cap, local_experts * cap
        num_in, num_out = len(IN_SPLIT), len(OUT_SPLIT)
        unit = d_model // sum(IN_SPLIT)
        kc = unit * max(IN_SPLIT)
        nw = d_model // sum(OUT_SPLIT) * max(OUT_SPLIT)
        chips, half = num_dev // 2, num_tokens // 2
        dma = pltpu.SemaphoreType.DMA
        any_spec = pl.BlockSpec(memory_space=pl.ANY)
        return pl.pallas_call(
            functools.partial(moe_kernel, cap),
            out_shape=pltpu.VMEM((num_tokens, d_model), BF16),
            in_specs=[any_spec] * 6,
            out_specs=pl.BlockSpec(memory_space=pltpu.VMEM),
            scratch_shapes=[
                pltpu.VMEM(routes.shape[::-1], jnp.int32),
                pltpu.VMEM(w_router.shape[::-1], BF16),
                pltpu.VMEM((num_dev, num_tokens, d_model), BF16),
                pltpu.VMEM((local_experts, rows, kc), F32),
                pltpu.VMEM((local_experts, rows, d_expert), F32),
                pltpu.VMEM((local_experts, rows, d_expert), F32),
                pltpu.VMEM((local_experts, rows, d_expert), BF16),
                pltpu.VMEM((RING * 2 * d_expert // COLS * unit, COLS), BF16),
                pltpu.VMEM((num_dev, slots, num_tokens), BF16),
                pltpu.VMEM((num_dev, 3 * num_tokens, slots), BF16),
                pltpu.VMEM((num_dev, local_experts, num_tokens), F32),
                pltpu.VMEM((num_dev, local_experts, num_tokens), F32),
                pltpu.VMEM((num_dev, local_experts, num_tokens), F32),
                pltpu.VMEM((num_dev, local_experts, num_tokens), F32),
                pltpu.VMEM((OWN_SLOTS, chips, num_tokens, nw), F32),
                pltpu.VMEM((2, chips, num_tokens, nw), F32),
                pltpu.VMEM((num_out, chips, num_tokens, nw), F32),
                pltpu.VMEM((num_out, 2, half, nw), F32),
                pltpu.VMEM((num_out, 2, num_tokens, nw), F32),
                dma, dma, dma, dma((num_in * local_experts // EXP_GROUP,)), dma((num_out,)),
                dma, dma((num_in, 5)), dma, dma, dma, dma,
                dma((2,)), dma((num_out, 2)), dma((OWN_SLOTS,)), dma((num_out, 2)), dma((num_out,)),
            ],
            compiler_params=pltpu.CompilerParams(
                collective_id=0, has_side_effects=True, vmem_limit_bytes=65_000_000
            ),
            name="moe_step",
        )(tokens, routes.T, w_router.T, w_one, w_three, w_two)

    return jax.shard_map(
        device_step, mesh=mesh,
        in_specs=(row_spec, row_spec, P(None, None), expert_spec, expert_spec, expert_spec),
        out_specs=row_spec, check_vma=False,
    )
```
